32 devices in a mesh: pop: 8 (over z, y), merge: 4 (over x, core).
Axes of the slice: x: 2, y: 2, z: 4, core: 2. Of those that a mesh axis runs over, the one named last changes fastest.
Arguments:
- slab: float32 [256, 256, 4096], P('pop', 'merge'), may hold values from -6 to 6
- sample_counts: int32 [2], replicated, may hold values from 160 to 255
- mode_rows_one: float32 [96, 256], replicated, may hold values from -0.375 to 0.375
- mode_rows_two: float32 [96, 256], replicated, may hold values from -0.375 to 0.375
- merge_tensor: float32 [96, 96, 96], replicated, may hold values from -0.0625 to 0.0625
- ancestral_modes: float32 [96, 256], replicated, may hold values from -0.625 to 0.625
Outputs:
- merged: float32 [4096, 256], P(('pop', 'merge'))
The draws below stay inside these ranges and needn't reach their ends.
All inputs are finite; a program needn't handle non-finite values.
Results may differ from the reference program's by a relative error of at most 0.000076.
Values sent between devices are 32-bit elements; how exact they have to be, the bound alone decides.
No kernel may reach another device: no remote copies, remote signals or barrier semaphores. Data moves between devices by JAX's collectives and lax.ppermute only.
A program may use at most 128 MiB of HBM per device.

```python
import jax
import jax.numpy as jnp
from jax import lax

N1 = 256
N2 = 256
NA = 256
K = 96
COLS = 4096


def level_of(key, shape, split, low, top_value):
    factor_of, own = 1.0, jax.random.fold_in(key, 6)
    for position, shards_of in split:
        draws = jnp.exp(jax.random.uniform(jax.random.fold_in(own, position), (shards_of,), jnp.float32, low / len(split), top_value / len(split)))
        factor_of = factor_of * jnp.repeat(draws, shape[position] // shards_of).reshape([-1 if axis == position else 1 for axis in range(len(shape))])
    return factor_of


def normal_values(key, dims, scale, limit, pieces=(), held_as=jnp.bfloat16):
    result = jax.random.normal(key, dims, jnp.float32) * scale
    if len(pieces) > 0:
        result = level_of(key, dims, pieces, -0.22, 0.18) * result
    return jnp.clip(result, min=-limit, max=limit).astype(held_as)


def setup_inputs(seed: int = 0) -> dict:
    splits = jax.random.split(jax.random.key(seed), 7)
    return {
        "slab": normal_values(splits[0], (N1, N2, COLS), 1.0, 6.0, ((0, 8), (1, 4)), jnp.float32),
        "sample_counts": jax.random.randint(splits[1], (2,), 5 * min(N1, N2) // 8, min(N1, N2)).astype(jnp.int32),
        "mode_rows_one": normal_values(splits[2], (K, N1), N1 ** -0.5, 0.375, (), jnp.float32),
        "mode_rows_two": normal_values(splits[3], (K, N2), N2 ** -0.5, 0.375, (), jnp.float32),
        "merge_tensor": normal_values(splits[4], (K, K, K), (K * K) ** -0.5, 0.0625, (), jnp.float32),
        "ancestral_modes": normal_values(splits[5], (K, NA), K ** -0.5, 0.625, (), jnp.float32),
    }


branch_one = 0.00025
branch_two = 0.0004


def prepared(rows, count, length, branch):
    order = jnp.arange(rows.shape[0], dtype=jnp.float32)
    decay = jnp.exp(-branch * order * (order + 1.0) / 2.0).astype(rows.dtype)
    keep = jnp.arange(length, dtype=jnp.int32) <= count
    return jnp.where(keep[None, :], rows, jnp.zeros_like(rows)) * decay[:, None]


def reference(slab, sample_counts, mode_rows_one, mode_rows_two, merge_tensor, ancestral_modes):
    high = lax.Precision.HIGHEST
    proj_one = prepared(mode_rows_one, sample_counts[0], N1, branch_one)
    proj_two = prepared(mode_rows_two, sample_counts[1], N2, branch_two)
    modal = jnp.einsum("ka,abc->kbc", proj_one, slab, precision=high)
    folded = jnp.einsum("mnj,nb->jmb", merge_tensor, proj_two, precision=high)
    summed = lax.dot_general(modal.reshape(K * N2, COLS), folded.reshape(K, K * N2), (((0,), (1,)), ((), ())), precision=high)
    return jnp.dot(summed, ancestral_modes, precision=high)
```

```python
import jax
import jax.numpy as jnp
from jax import lax
from jax.experimental import pallas as pl
from jax.experimental.pallas import tpu as pltpu
from jax.sharding import PartitionSpec as P

branch_one = 0.00025
branch_two = 0.0004
AXES = ("pop", "merge")
LANES = 128


def prepared(rows, count, branch):
    order = jnp.arange(rows.shape[0], dtype=jnp.float32)
    decay = jnp.exp(-branch * order * (order + 1.0) / 2.0)
    keep = jnp.arange(rows.shape[1], dtype=jnp.int32) <= count
    return jnp.where(keep[None, :], rows, jnp.zeros_like(rows)) * decay[:, None]


def split(value):
    high = lax.reduce_precision(value, 8, 7)
    return high.astype(jnp.bfloat16), (value - high).astype(jnp.bfloat16)


def split_block(value):
    high = value.astype(jnp.bfloat16)
    return high, (value - high.astype(jnp.float32)).astype(jnp.bfloat16)


def partial_sums(slab, weave, pops, merges, wide):
    rows, cols = slab.shape
    modes = weave.shape[0] // 2
    per = cols // (pops * merges)

    def body(where, slab_ref, weave_ref, out_ref):
        high, low = split_block(slab_ref[...])
        two = jnp.dot(weave_ref[...], high, preferred_element_type=jnp.float32)
        one = jnp.dot(weave_ref[:modes], low, preferred_element_type=jnp.float32)
        value = two[:modes] + (two[modes:] + one)
        for m in range(merges):
            out_ref[0, jnp.bitwise_xor(where[1], m)] = value[:, m * per : (m + 1) * per]

    return pl.pallas_call(
        body,
        out_shape=jax.ShapeDtypeStruct((pops, merges, modes, per), jnp.float32),
        grid_spec=pltpu.PrefetchScalarGridSpec(
            num_scalar_prefetch=1,
            grid=(pops,),
            in_specs=[
                pl.BlockSpec((rows, merges * per), lambda i, where: (0, jnp.bitwise_xor(i, where[0]))),
                pl.BlockSpec(weave.shape, lambda i, where: (0, 0)),
            ],
            out_specs=pl.BlockSpec((1, merges, modes, per), lambda i, where: (i, 0, 0, 0)),
        ),
        compiler_params=pltpu.CompilerParams(vmem_limit_bytes=48 * 1024 * 1024),
    )(jnp.stack([lax.axis_index("pop"), lax.axis_index("merge")]).astype(jnp.int32), slab, weave)


def scatter_sum(value, devices):
    bits = [1 << k for k in reversed(range(devices.bit_length() - 1))]
    value = value.reshape((2,) * len(bits) + value.shape[-2:])
    for group in ([bits[-1]], bits[1:-1], [bits[0]]):
        combos = [0]
        for bit in group:
            combos = combos + [c | bit for c in combos]

        def piece(c):
            return value[tuple((1 if c & b else 0) if b in group else slice(None) for b in bits)]

        sent = [
            lax.ppermute(piece(c), AXES, [(i, i ^ c) for i in range(devices)]) for c in combos[1:]
        ]
        total = piece(0)
        for part in sent:
            total = total + part
        value = total
        bits = [b for b in bits if b not in group]
    return value


def on_device(pops, merges):
    devices = pops * merges

    def run(slab, sample_counts, mode_rows_one, mode_rows_two, merge_tensor, ancestral_modes):
        high = lax.Precision.HIGHEST
        modes = mode_rows_one.shape[0]
        proj_one = prepared(mode_rows_one, sample_counts[0], branch_one)
        proj_two = prepared(mode_rows_two, sample_counts[1], branch_two)
        rows_one, rows_two, cols = slab.shape
        begin_one = lax.axis_index("pop") * rows_one
        begin_two = lax.axis_index("merge") * rows_two
        local_one = lax.dynamic_slice_in_dim(proj_one, begin_one, rows_one, 1)
        local_two = lax.dynamic_slice_in_dim(proj_two, begin_two, rows_two, 1)
        folded_local = jnp.einsum("mnj,nb->jmb", merge_tensor, local_two, precision=high)
        weave = jnp.einsum("ma,jmb->jab", local_one, folded_local, precision=high)
        weave = weave.reshape(modes, rows_one * rows_two)
        flat_slab = slab.reshape(rows_one * rows_two, cols)
        two_power = devices & (devices - 1) == 0 and pops > 2 and merges > 1
        if two_power and cols % (devices * LANES) == 0:
            parts = partial_sums(flat_slab, jnp.concatenate(split(weave)), pops, merges, 0)
            summed = scatter_sum(parts, devices)
        else:
            summed = lax.psum_scatter(
                lax.dot_general(weave, flat_slab, (((1,), (0,)), ((), ())), precision=high),
                AXES,
                scatter_dimension=1,
                tiled=True,
            )
        return lax.dot_general(summed, ancestral_modes, (((0,), (0,)), ((), ())), precision=high)

    return run


def solution(mesh):
    in_specs = (P("pop", "merge", None), P(), P(), P(), P(), P())
    out_specs = P(AXES, None)
    run = on_device(mesh.shape["pop"], mesh.shape["merge"])
    return jax.shard_map(run, mesh=mesh, in_specs=in_specs, out_specs=out_specs, check_vma=False)
```

```python
import jax
import jax.numpy as jnp
from jax import lax
from jax.experimental import pallas as pl
from jax.experimental.pallas import tpu as pltpu
from jax.sharding import PartitionSpec as P

branch_one = 0.00025
branch_two = 0.0004
AXES = ("pop", "merge")
LANES = 128
SUBLANES = 8


def prepared(rows, count, branch):
    order = jnp.arange(rows.shape[0], dtype=jnp.float32)
    decay = jnp.exp(-branch * order * (order + 1.0) / 2.0)
    keep = jnp.arange(rows.shape[1], dtype=jnp.int32) <= count
    return jnp.where(keep[None, :], rows, jnp.zeros_like(rows)) * decay[:, None]


def split(value):
    high = value.astype(jnp.bfloat16)
    return high, (value - high.astype(jnp.float32)).astype(jnp.bfloat16)


def product(stacked, count, value):
    high, low = split(value)
    two = jnp.dot(stacked, high, preferred_element_type=jnp.float32)
    one = jnp.dot(stacked[:count], low, preferred_element_type=jnp.float32)
    return two[:count] + (two[count:] + one)


def partial_sums(slab, counts, rows_one, rows_two, merge_tensor, local_one, local_two, pops, merges):
    rows, cols = slab.shape
    modes = rows_one.shape[0]
    per = cols // (pops * merges)
    wide = merges * per
    step_one = local_two + SUBLANES
    padded = pl.cdiv(modes, LANES) * LANES

    def body(
        counts_ref, one_ref, two_ref, tensor_ref, slab_ref, out_ref,
        tensor_buf, slab_buf, rows_buf, folded_ref, woven_ref, weave_ref, tensor_sem, slab_sems,
    ):
        pop = lax.axis_index("pop")
        merge = lax.axis_index("merge")
        tensor_copy = pltpu.make_async_copy(tensor_ref, tensor_buf, tensor_sem)
        tensor_copy.start()

        def slab_copy(i):
            at = pl.multiple_of(jnp.bitwise_xor(i, pop) * wide, LANES)
            return pltpu.make_async_copy(
                slab_ref.at[:, pl.ds(at, wide)], slab_buf.at[i], slab_sems.at[i]
            )

        def local(ref, count, branch, begin, size):
            full = jnp.concatenate(
                [ref[...], jnp.zeros((padded - modes, ref.shape[1]), jnp.float32)], axis=0
            )
            rows_buf[: ref.shape[1]] = full.T
            mine = rows_buf[pl.ds(pl.multiple_of(begin, SUBLANES), size)]
            order = lax.broadcasted_iota(jnp.int32, mine.shape, 1).astype(jnp.float32)
            decay = jnp.exp(-branch * order * (order + 1.0) / 2.0)
            entry = lax.broadcasted_iota(jnp.int32, mine.shape, 0) + begin
            mine = jnp.where(entry <= count, mine, 0.0) * decay
            return jnp.concatenate(split(mine[:, :modes]), axis=0)

        proj_two = local(two_ref, counts_ref[1], branch_two, merge * local_two, local_two)
        proj_one = local(one_ref, counts_ref[0], branch_one, pop * local_one, local_one)
        tensor_copy.wait()
        for i in range(pops):
            slab_copy(i).start()

        def fold(m, carry):
            at = pl.multiple_of(m * step_one, SUBLANES)
            folded_ref[pl.ds(at, local_two), :modes] = product(proj_two, local_two, tensor_buf[m])
            return carry

        lax.fori_loop(0, modes, fold, 0, unroll=8)

        def weave(b, carry):
            value = folded_ref[pl.ds(b, modes, stride=step_one), :]
            woven_ref[pl.ds(b, local_one, stride=step_one), :] = product(proj_one, local_one, value)
            return carry

        lax.fori_loop(0, local_two, weave, 0, unroll=8)

        group = LANES // local_two
        for q in range(local_one // group):
            value = jnp.concatenate(
                [woven_ref[pl.ds((q * group + k) * step_one, local_two), :] for k in range(group)],
                axis=0,
            )
            high, low = split(value.T[:modes])
            weave_ref[:modes, q * LANES : (q + 1) * LANES] = high
            weave_ref[modes:, q * LANES : (q + 1) * LANES] = low

        def block(i, carry):
            slab_copy(i).wait()
            value = product(weave_ref[...], modes, slab_buf[i])
            for m in range(merges):
                out_ref[i, jnp.bitwise_xor(merge, m)] = value[:, m * per : (m + 1) * per]
            return carry

        lax.fori_loop(0, pops, block, 0)

    vmem = pl.BlockSpec(memory_space=pltpu.VMEM)
    hbm = pl.BlockSpec(memory_space=pl.ANY)
    return pl.pallas_call(
        body,
        out_shape=jax.ShapeDtypeStruct((pops, merges, modes, per), jnp.float32),
        in_specs=[pl.BlockSpec(memory_space=pltpu.SMEM), vmem, vmem, hbm, hbm],
        out_specs=vmem,
        scratch_shapes=[
            pltpu.VMEM(merge_tensor.shape, jnp.float32),
            pltpu.VMEM((pops, rows, wide), jnp.float32),
            pltpu.VMEM((max(rows_one.shape[1], rows_two.shape[1]), padded), jnp.float32),
            pltpu.VMEM((modes * step_one, padded), jnp.float32),
            pltpu.VMEM((local_one * step_one, padded), jnp.float32),
            pltpu.VMEM((2 * modes, rows), jnp.bfloat16),
            pltpu.SemaphoreType.DMA,
            pltpu.SemaphoreType.DMA((pops,)),
        ],
        compiler_params=pltpu.CompilerParams(vmem_limit_bytes=56 * 1024 * 1024),
    )(counts, rows_one, rows_two, merge_tensor, slab)


def scatter_sum(value, devices):
    bits = [1 << k for k in reversed(range(devices.bit_length() - 1))]
    value = value.reshape((2,) * len(bits) + value.shape[-2:])
    for group in ([bits[-1]], bits[1:-1], [bits[0]]):
        combos = [0]
        for bit in group:
            combos = combos + [c | bit for c in combos]

        def piece(c):
            return value[tuple((1 if c & b else 0) if b in group else slice(None) for b in bits)]

        sent = [
            lax.ppermute(piece(c), AXES, [(i, i ^ c) for i in range(devices)]) for c in combos[1:]
        ]
        total = piece(0)
        for part in sent:
            total = total + part
        value = total
        bits = [b for b in bits if b not in group]
    return value


def on_device(pops, merges):
    devices = pops * merges

    def run(slab, sample_counts, mode_rows_one, mode_rows_two, merge_tensor, ancestral_modes):
        high = lax.Precision.HIGHEST
        modes = mode_rows_one.shape[0]
        local_one, local_two, cols = slab.shape
        flat_slab = slab.reshape(local_one * local_two, cols)
        two_power = devices & (devices - 1) == 0 and pops > 2 and merges > 1
        tiles = local_one % SUBLANES == 0 and local_two % SUBLANES == 0 and LANES % local_two == 0
        if two_power and tiles and cols % (devices * LANES) == 0:
            parts = partial_sums(
                flat_slab, sample_counts, mode_rows_one, mode_rows_two, merge_tensor,
                local_one, local_two, pops, merges,
            )
            summed = scatter_sum(parts, devices)
        else:
            proj_one = prepared(mode_rows_one, sample_counts[0], branch_one)
            proj_two = prepared(mode_rows_two, sample_counts[1], branch_two)
            begin_one = lax.axis_index("pop") * local_one
            begin_two = lax.axis_index("merge") * local_two
            mine_one = lax.dynamic_slice_in_dim(proj_one, begin_one, local_one, 1)
            mine_two = lax.dynamic_slice_in_dim(proj_two, begin_two, local_two, 1)
            folded = jnp.einsum("mnj,nb->jmb", merge_tensor, mine_two, precision=high)
            weave = jnp.einsum("ma,jmb->jab", mine_one, folded, precision=high)
            weave = weave.reshape(modes, local_one * local_two)
            summed = lax.psum_scatter(
                lax.dot_general(weave, flat_slab, (((1,), (0,)), ((), ())), precision=high),
                AXES,
                scatter_dimension=1,
                tiled=True,
            )
        return lax.dot_general(summed, ancestral_modes, (((0,), (0,)), ((), ())), precision=high)

    return run


def solution(mesh):
    in_specs = (P("pop", "merge", None), P(), P(), P(), P(), P())
    out_specs = P(AXES, None)
    run = on_device(mesh.shape["pop"], mesh.shape["merge"])
    return jax.shard_map(run, mesh=mesh, in_specs=in_specs, out_specs=out_specs, check_vma=False)
```

```python
import jax
import jax.numpy as jnp
from jax import lax
from jax.experimental import pallas as pl
from jax.experimental.pallas import tpu as pltpu
from jax.sharding import PartitionSpec as P

branch_one = 0.00025
branch_two = 0.0004
AXES = ("pop", "merge")
LANES = 128
SUBLANES = 8
CHUNKS = 3
VMEM = 56 * 1024 * 1024


def prepared(rows, count, branch):
    order = jnp.arange(rows.shape[0], dtype=jnp.float32)
    decay = jnp.exp(-branch * order * (order + 1.0) / 2.0)
    keep = jnp.arange(rows.shape[1], dtype=jnp.int32) <= count
    return jnp.where(keep[None, :], rows, jnp.zeros_like(rows)) * decay[:, None]


def split(value):
    high = value.astype(jnp.bfloat16)
    return high, (value - high.astype(jnp.float32)).astype(jnp.bfloat16)


def product(stacked, count, value):
    high, low = split(value)
    two = jnp.dot(stacked, high, preferred_element_type=jnp.float32)
    one = jnp.dot(stacked[:count], low, preferred_element_type=jnp.float32)
    return two[:count] + (two[count:] + one)


def store(out_ref, i, merge, value, merges, per):
    for m in range(merges):
        r = jnp.bitwise_xor(merge, m)
        out_ref[r % 2, i, r // 2] = value[:, m * per : (m + 1) * per]


def partial_sums(slab, counts, rows_one, rows_two, merge_tensor, local_one, local_two, pops, merges):
    rows, cols = slab.shape
    modes = rows_one.shape[0]
    per = cols // (pops * merges)
    wide = merges * per
    step_one = local_two + SUBLANES
    padded = pl.cdiv(modes, LANES) * LANES

    def body(
        counts_ref, one_ref, two_ref, tensor_ref, slab_ref, out_ref,
        one_buf, two_buf, tensor_buf, slab_buf, rows_buf, folded_ref, woven_ref, weave_ref,
        rows_sems, tensor_sems, slab_sems,
    ):
        pop = lax.axis_index("pop")
        merge = lax.axis_index("merge")
        chunk = modes // CHUNKS

        def tensor_copy(k):
            at = pl.ds(k * chunk, chunk)
            return pltpu.make_async_copy(tensor_ref.at[at], tensor_buf.at[at], tensor_sems.at[k])

        two_copy = pltpu.make_async_copy(two_ref, two_buf, rows_sems.at[0])
        one_copy = pltpu.make_async_copy(one_ref, one_buf, rows_sems.at[1])
        two_copy.start()
        one_copy.start()
        for k in range(CHUNKS):
            tensor_copy(k).start()

        def slab_copy(i):
            at = pl.multiple_of(jnp.bitwise_xor(i, pop) * wide, LANES)
            return pltpu.make_async_copy(
                slab_ref.at[:, pl.ds(at, wide)], slab_buf.at[i], slab_sems.at[i]
            )

        slab_copy(0).start()

        def local(ref, count, branch, begin, size):
            full = jnp.concatenate(
                [ref[...], jnp.zeros((padded - modes, ref.shape[1]), jnp.float32)], axis=0
            )
            rows_buf[: ref.shape[1]] = full.T
            mine = rows_buf[pl.ds(pl.multiple_of(begin, SUBLANES), size)]
            order = lax.broadcasted_iota(jnp.int32, mine.shape, 1).astype(jnp.float32)
            decay = jnp.exp(-branch * order * (order + 1.0) / 2.0)
            entry = lax.broadcasted_iota(jnp.int32, mine.shape, 0) + begin
            mine = jnp.where(entry <= count, mine, 0.0) * decay
            return jnp.concatenate(split(mine[:, :modes]), axis=0)

        two_copy.wait()
        proj_two = local(two_buf, counts_ref[1], branch_two, merge * local_two, local_two)
        one_copy.wait()
        proj_one = local(one_buf, counts_ref[0], branch_one, pop * local_one, local_one)

        def fold(m, carry):
            at = pl.multiple_of(m * step_one, SUBLANES)
            folded_ref[pl.ds(at, local_two), :modes] = product(proj_two, local_two, tensor_buf[m])
            return carry

        for k in range(CHUNKS):
            tensor_copy(k).wait()
            for i in range(1 + k * (pops - 1) // CHUNKS, 1 + (k + 1) * (pops - 1) // CHUNKS):
                slab_copy(i).start()
            lax.fori_loop(k * chunk, (k + 1) * chunk, fold, 0, unroll=32)

        def weave(b, carry):
            value = folded_ref[pl.ds(b, modes, stride=step_one), :]
            woven_ref[pl.ds(b, local_one, stride=step_one), :] = product(proj_one, local_one, value)
            return carry

        lax.fori_loop(0, local_two, weave, 0, unroll=32)

        group = LANES // local_two
        for q in range(local_one // group):
            value = jnp.concatenate(
                [woven_ref[pl.ds((q * group + k) * step_one, local_two), :] for k in range(group)],
                axis=0,
            )
            high, low = split(value.T[:modes])
            weave_ref[:modes, q * LANES : (q + 1) * LANES] = high
            weave_ref[modes:, q * LANES : (q + 1) * LANES] = low

        for i in range(pops):
            slab_copy(i).wait()
            store(out_ref, i, merge, product(weave_ref[...], modes, slab_buf[i]), merges, per)

    vmem = pl.BlockSpec(memory_space=pltpu.VMEM)
    hbm = pl.BlockSpec(memory_space=pltpu.HBM)
    return pl.pallas_call(
        body,
        out_shape=pltpu.VMEM((2, pops, merges // 2, modes, per), jnp.float32),
        in_specs=[pl.BlockSpec(memory_space=pltpu.SMEM), hbm, hbm, hbm, hbm],
        out_specs=vmem,
        scratch_shapes=[
            pltpu.VMEM(rows_one.shape, jnp.float32),
            pltpu.VMEM(rows_two.shape, jnp.float32),
            pltpu.VMEM(merge_tensor.shape, jnp.float32),
            pltpu.VMEM((pops, rows, wide), jnp.float32),
            pltpu.VMEM((max(rows_one.shape[1], rows_two.shape[1]), padded), jnp.float32),
            pltpu.VMEM((modes * step_one, padded), jnp.float32),
            pltpu.VMEM((local_one * step_one, padded), jnp.float32),
            pltpu.VMEM((2 * modes, rows), jnp.bfloat16),
            pltpu.SemaphoreType.DMA((2,)),
            pltpu.SemaphoreType.DMA((CHUNKS,)),
            pltpu.SemaphoreType.DMA((pops,)),
        ],
        compiler_params=pltpu.CompilerParams(vmem_limit_bytes=VMEM),
    )(counts, rows_one, rows_two, merge_tensor, slab)


def direct_sum(value, bits, group, devices):
    combos = [0]
    for bit in group:
        combos = combos + [c | bit for c in combos]

    def piece(c):
        return value[tuple((1 if c & b else 0) if b in group else slice(None) for b in bits)]

    sent = [to(piece(c), c, devices) for c in combos[1:]]
    total = piece(0)
    for part in sent:
        total = total + part
    return total


def to(value, bit, devices):
    return lax.ppermute(value, AXES, [(i, i ^ bit) for i in range(devices)])


def on_device(pops, merges):
    devices = pops * merges

    def run(slab, sample_counts, mode_rows_one, mode_rows_two, merge_tensor, ancestral_modes):
        high = lax.Precision.HIGHEST
        modes = mode_rows_one.shape[0]
        local_one, local_two, cols = slab.shape
        flat_slab = slab.reshape(local_one * local_two, cols)
        two_power = devices & (devices - 1) == 0 and pops > 4 and merges > 1
        tiles = local_one % SUBLANES == 0 and local_two % SUBLANES == 0 and LANES % local_two == 0 and modes % CHUNKS == 0
        if two_power and tiles and cols % (devices * LANES) == 0:
            parts = partial_sums(
                flat_slab, sample_counts, mode_rows_one, mode_rows_two, merge_tensor,
                local_one, local_two, pops, merges,
            )
            summed = parts[0] + to(parts[1], 1, devices)
            bits = [1 << k for k in reversed(range(1, devices.bit_length() - 1))]
            summed = summed.reshape((2,) * len(bits) + summed.shape[-2:])
            summed = direct_sum(summed, bits, bits[1:], devices)
            summed = direct_sum(summed, bits[:1], bits[:1], devices)
        else:
            proj_one = prepared(mode_rows_one, sample_counts[0], branch_one)
            proj_two = prepared(mode_rows_two, sample_counts[1], branch_two)
            begin_one = lax.axis_index("pop") * local_one
            begin_two = lax.axis_index("merge") * local_two
            mine_one = lax.dynamic_slice_in_dim(proj_one, begin_one, local_one, 1)
            mine_two = lax.dynamic_slice_in_dim(proj_two, begin_two, local_two, 1)
            folded = jnp.einsum("mnj,nb->jmb", merge_tensor, mine_two, precision=high)
            weave = jnp.einsum("ma,jmb->jab", mine_one, folded, precision=high)
            weave = weave.reshape(modes, local_one * local_two)
            summed = lax.psum_scatter(
                lax.dot_general(weave, flat_slab, (((1,), (0,)), ((), ())), precision=high),
                AXES,
                scatter_dimension=1,
                tiled=True,
            )
        return lax.dot_general(summed, ancestral_modes, (((0,), (0,)), ((), ())), precision=high)

    return run


def solution(mesh):
    in_specs = (P("pop", "merge", None), P(), P(), P(), P(), P())
    out_specs = P(AXES, None)
    run = on_device(mesh.shape["pop"], mesh.shape["merge"])
    return jax.shard_map(run, mesh=mesh, in_specs=in_specs, out_specs=out_specs, check_vma=False)
```

```python
import jax
import jax.numpy as jnp
from jax import lax
from jax.experimental import pallas as pl
from jax.experimental.pallas import tpu as pltpu
from jax.sharding import PartitionSpec as P


branch_one = 0.00025
branch_two = 0.0004
AXES = ("pop", "merge")
LANES = 128
SUBLANES = 8
CHUNKS = 3
AHEAD = 5
VMEM = 56 * 1024 * 1024


def prepared(rows, count, branch):
    order = jnp.arange(rows.shape[0], dtype=jnp.float32)
    decay = jnp.exp(-branch * order * (order + 1.0) / 2.0)
    keep = jnp.arange(rows.shape[1], dtype=jnp.int32) <= count
    return jnp.where(keep[None, :], rows, jnp.zeros_like(rows)) * decay[:, None]


def split(value):
    high = value.astype(jnp.bfloat16)
    return high, (value - high.astype(jnp.float32)).astype(jnp.bfloat16)


def product(stacked, count, value):
    high, low = split(value)
    two = jnp.dot(stacked, high, preferred_element_type=jnp.float32)
    one = jnp.dot(stacked[:count], low, preferred_element_type=jnp.float32)
    return two[:count] + (two[count:] + one)


def store(out_ref, i, merge, value, merges, per):
    for m in range(merges):
        r = jnp.bitwise_xor(merge, m)
        out_ref[r % 2, i, r // 2] = value[:, m * per : (m + 1) * per]


def partial_sums(slab, counts, rows_one, rows_two, merge_tensor, local_one, local_two, pops, merges):
    rows, cols = slab.shape
    modes = rows_one.shape[0]
    per = cols // (pops * merges)
    wide = merges * per
    step_one = local_two + SUBLANES
    padded = pl.cdiv(modes, LANES) * LANES

    def body(
        counts_ref, one_ref, two_ref, tensor_ref, slab_ref, out_ref,
        one_buf, two_buf, tensor_buf, slab_buf, rows_buf, folded_ref, woven_ref, weave_ref,
        rows_sems, tensor_sems, slab_sems,
    ):
        pop = lax.axis_index("pop")
        merge = lax.axis_index("merge")
        chunk = modes // CHUNKS

        def tensor_copy(k):
            at = pl.ds(k * chunk, chunk)
            return pltpu.make_async_copy(tensor_ref.at[at], tensor_buf.at[at], tensor_sems.at[k])

        two_copy = pltpu.make_async_copy(two_ref, two_buf, rows_sems.at[0])
        one_copy = pltpu.make_async_copy(one_ref, one_buf, rows_sems.at[1])
        two_copy.start()
        one_copy.start()
        for k in range(CHUNKS):
            tensor_copy(k).start()

        def slab_copy(i):
            at = pl.multiple_of(jnp.bitwise_xor(i, pop) * wide, LANES)
            return pltpu.make_async_copy(
                slab_ref.at[:, pl.ds(at, wide)], slab_buf.at[i], slab_sems.at[i]
            )

        slab_copy(0).start()

        def local(ref, count, branch, begin, size):
            full = jnp.concatenate(
                [ref[...], jnp.zeros((padded - modes, ref.shape[1]), jnp.float32)], axis=0
            )
            rows_buf[: ref.shape[1]] = full.T
            mine = rows_buf[pl.ds(pl.multiple_of(begin, SUBLANES), size)]
            order = lax.broadcasted_iota(jnp.int32, mine.shape, 1).astype(jnp.float32)
            decay = jnp.exp(-branch * order * (order + 1.0) / 2.0)
            entry = lax.broadcasted_iota(jnp.int32, mine.shape, 0) + begin
            mine = jnp.where(entry <= count, mine, 0.0) * decay
            return jnp.concatenate(split(mine[:, :modes]), axis=0)

        two_copy.wait()
        proj_two = local(two_buf, counts_ref[1], branch_two, merge * local_two, local_two)
        one_copy.wait()
        proj_one = local(one_buf, counts_ref[0], branch_one, pop * local_one, local_one)

        def fold(m, carry):
            at = pl.multiple_of(m * step_one, SUBLANES)
            folded_ref[pl.ds(at, local_two), :modes] = product(proj_two, local_two, tensor_buf[m])
            return carry

        for k in range(CHUNKS):
            tensor_copy(k).wait()
            for i in range(1 + k * (AHEAD - 1) // CHUNKS, 1 + (k + 1) * (AHEAD - 1) // CHUNKS):
                slab_copy(i).start()
            lax.fori_loop(k * chunk, (k + 1) * chunk, fold, 0, unroll=32)

        def weave(b, carry):
            value = folded_ref[pl.ds(b, modes, stride=step_one), :]
            woven_ref[pl.ds(b, local_one, stride=step_one), :] = product(proj_one, local_one, value)
            return carry

        lax.fori_loop(0, local_two, weave, 0, unroll=64)

        group = LANES // local_two
        for q in range(local_one // group):
            value = jnp.concatenate(
                [woven_ref[pl.ds((q * group + k) * step_one, local_two), :] for k in range(group)],
                axis=0,
            )
            high, low = split(value.T[:modes])
            weave_ref[:modes, q * LANES : (q + 1) * LANES] = high
            weave_ref[modes:, q * LANES : (q + 1) * LANES] = low

        for i in range(pops):
            slab_copy(i).wait()
            if i + AHEAD < pops:
                slab_copy(i + AHEAD).start()
            store(out_ref, i, merge, product(weave_ref[...], modes, slab_buf[i]), merges, per)

    vmem = pl.BlockSpec(memory_space=pltpu.VMEM)
    hbm = pl.BlockSpec(memory_space=pltpu.HBM)
    return pl.pallas_call(
        body,
        out_shape=pltpu.VMEM((2, pops, merges // 2, modes, per), jnp.float32),
        in_specs=[pl.BlockSpec(memory_space=pltpu.SMEM), hbm, hbm, hbm, hbm],
        out_specs=vmem,
        scratch_shapes=[
            pltpu.VMEM(rows_one.shape, jnp.float32),
            pltpu.VMEM(rows_two.shape, jnp.float32),
            pltpu.VMEM(merge_tensor.shape, jnp.float32),
            pltpu.VMEM((pops, rows, wide), jnp.float32),
            pltpu.VMEM((max(rows_one.shape[1], rows_two.shape[1]), padded), jnp.float32),
            pltpu.VMEM((modes * step_one, padded), jnp.float32),
            pltpu.VMEM((local_one * step_one, padded), jnp.float32),
            pltpu.VMEM((2 * modes, rows), jnp.bfloat16),
            pltpu.SemaphoreType.DMA((2,)),
            pltpu.SemaphoreType.DMA((CHUNKS,)),
            pltpu.SemaphoreType.DMA((pops,)),
        ],
        compiler_params=pltpu.CompilerParams(vmem_limit_bytes=VMEM),
    )(counts, rows_one, rows_two, merge_tensor, slab)


def direct_sum(value, bits, group, devices):
    combos = [0]
    for bit in group:
        combos = combos + [c | bit for c in combos]

    def piece(c):
        return value[tuple((1 if c & b else 0) if b in group else slice(None) for b in bits)]

    sent = []
    for c in combos[1:]:
        sent.append(to(piece(c), c, devices))
    total = piece(0)
    for part in sent:
        total = total + part
    return total


def to(value, bit, devices):
    return lax.ppermute(value, AXES, [(i, i ^ bit) for i in range(devices)])


def on_device(pops, merges):
    devices = pops * merges

    def run(slab, sample_counts, mode_rows_one, mode_rows_two, merge_tensor, ancestral_modes):
        high = lax.Precision.HIGHEST
        modes = mode_rows_one.shape[0]
        local_one, local_two, cols = slab.shape
        flat_slab = slab.reshape(local_one * local_two, cols)
        two_power = devices & (devices - 1) == 0 and pops > 4 and merges > 1
        tiles = local_one % SUBLANES == 0 and local_two % SUBLANES == 0 and LANES % local_two == 0 and modes % CHUNKS == 0
        if two_power and tiles and pops > AHEAD and cols % (devices * LANES) == 0:
            parts = partial_sums(
                flat_slab, sample_counts, mode_rows_one, mode_rows_two, merge_tensor,
                local_one, local_two, pops, merges,
            )
            summed = parts[0] + to(parts[1], 1, devices)
            bits = [1 << k for k in reversed(range(1, devices.bit_length() - 1))]
            summed = summed.reshape((2,) * len(bits) + summed.shape[-2:])
            summed = direct_sum(summed, bits, bits[1:], devices)
            summed = direct_sum(summed, bits[:1], bits[:1], devices)
        else:
            proj_one = prepared(mode_rows_one, sample_counts[0], branch_one)
            proj_two = prepared(mode_rows_two, sample_counts[1], branch_two)
            begin_one = lax.axis_index("pop") * local_one
            begin_two = lax.axis_index("merge") * local_two
            mine_one = lax.dynamic_slice_in_dim(proj_one, begin_one, local_one, 1)
            mine_two = lax.dynamic_slice_in_dim(proj_two, begin_two, local_two, 1)
            folded = jnp.einsum("mnj,nb->jmb", merge_tensor, mine_two, precision=high)
            weave = jnp.einsum("ma,jmb->jab", mine_one, folded, precision=high)
            weave = weave.reshape(modes, local_one * local_two)
            summed = lax.psum_scatter(
                lax.dot_general(weave, flat_slab, (((1,), (0,)), ((), ())), precision=high),
                AXES,
                scatter_dimension=1,
                tiled=True,
            )
        return lax.dot_general(summed, ancestral_modes, (((0,), (0,)), ((), ())), precision=high)

    return run


def solution(mesh):
    in_specs = (P("pop", "merge", None), P(), P(), P(), P(), P())
    out_specs = P(AXES, None)
    run = on_device(mesh.shape["pop"], mesh.shape["merge"])
    return jax.shard_map(run, mesh=mesh, in_specs=in_specs, out_specs=out_specs, check_vma=False)
```
